32 devices in a mesh: prow: 8 (over z, y), pcol: 4 (over x, core).
Axes of the slice: x: 2, y: 2, z: 4, core: 2. Of those that a mesh axis runs over, the one named last changes fastest.
Arguments:
- inverse_block: bfloat16 [2, 512, 512], P(None, 'prow', 'pcol'), may hold values from -1.75 to 1.75
- panel: bfloat16 [2, 512, 2048], P(None, ('prow', 'pcol')), may hold values from -0.5 to 0.5
- pattern: int32 [1, 4], replicated, may hold values 0 or 1
- diag_inverse: float32 [2, 512, 2048], P(None, None, 'pcol'), may hold values from -6 to 6
Outputs:
- offdiag: bfloat16 [2, 512, 2048], P(None, 'prow', 'pcol')
- diagonal: float32 [2, 512, 2048], P(None, None, 'pcol')
The draws below stay inside these ranges and needn't reach their ends.
All inputs are finite; a program needn't handle non-finite values.
Results may differ from the reference program's by a relative error of at most 0.0024.
Values may be sent and summed in bfloat16 or wider, within the bound.
A program may use at most 64 MiB of HBM per device.

```python
import jax
import jax.numpy as jnp

WIDTH = 512
NSUPER = 4
ORDER = 512
COLS = 2048
ANCESTORS = 1


def touch_ends(values, stream_key, smallest, high):
    longest = values.shape.index(max(values.shape))
    spots = []
    for shift in (0, 1):
        where = [jax.random.randint(jax.random.fold_in(stream_key, axis), (), 0, length) for axis, length in enumerate(values.shape)]
        where[longest] = (where[longest] + shift) % values.shape[longest]
        spots.append(tuple(where))
    return values.at[spots[0]].set(smallest).at[spots[1]].set(high)


def level_of(stream_key, dims, pieces, low, largest):
    factor_of = 1.0
    for dim, shards_of in pieces:
        draws = jax.random.uniform(jax.random.fold_in(jax.random.fold_in(stream_key, 6), dim), (shards_of,), jnp.float32, low / len(pieces), largest / len(pieces))
        factor_of = factor_of * jnp.repeat(jnp.exp(draws), dims[dim] // shards_of).reshape((-1,) + (1,) * (len(dims) - 1 - dim))
    return factor_of


def bell_draw(rng, shape, spread, most, pieces=(), held_as=jnp.bfloat16):
    array = jax.random.normal(rng, shape, jnp.float32) * spread
    if len(pieces) > 0:
        array = level_of(rng, shape, pieces, -0.22, 0.18) * array
    return jnp.clip(array, min=-most, max=most).astype(held_as)


def setup_inputs(seed: int = 0) -> dict:
    key_list = jax.random.split(jax.random.key(seed), 5)
    inverse_block = bell_draw(key_list[0], (2, ORDER, ORDER), 0.3, 1.75, ((1, 8), (2, 4)))
    panel = bell_draw(key_list[1], (2, ORDER, COLS), (1.8 * ORDER ** -0.5), 0.5, ((1, 32),))
    pattern = touch_ends((jax.random.randint(key_list[2], (ANCESTORS, NSUPER), 0, 3) < 2).astype(jnp.int32), jax.random.fold_in(key_list[2], 1), 0, 1)
    diag_inverse = bell_draw(key_list[3], (2, WIDTH, COLS), 1.0, 6.0, ((2, 4),), jnp.float32)
    return dict(inverse_block=inverse_block, panel=panel, pattern=pattern, diag_inverse=diag_inverse)


def complex_dot(left_real, left_imag, right_real, right_imag):
    real_part = jnp.dot(left_real, right_real, preferred_element_type=jnp.float32) - jnp.dot(left_imag, right_imag, preferred_element_type=jnp.float32)
    imag_part = jnp.dot(left_real, right_imag, preferred_element_type=jnp.float32) + jnp.dot(left_imag, right_real, preferred_element_type=jnp.float32)
    return real_part, imag_part


def reference(inverse_block, panel, pattern, diag_inverse):
    row_block = jnp.arange(ORDER, dtype=jnp.int32) // WIDTH
    col_block = jnp.arange(COLS, dtype=jnp.int32) // WIDTH
    keep_mask = pattern[row_block][:, col_block]
    masked = jnp.where(keep_mask[None] > 0, panel, jnp.zeros_like(panel))
    real_part, imag_part = complex_dot(inverse_block[0], inverse_block[1], masked[0], masked[1])
    keep_float = keep_mask.astype(jnp.float32)
    coupled = (jnp.stack([real_part, imag_part]) * keep_float[None]).astype(jnp.bfloat16)
    offdiag = -coupled
    blocks = []
    for member in range(NSUPER):
        lower_real = masked[0, :, member * WIDTH:(member + 1) * WIDTH]
        lower_imag = masked[1, :, member * WIDTH:(member + 1) * WIDTH]
        upper_real = coupled[0, :, member * WIDTH:(member + 1) * WIDTH]
        upper_imag = coupled[1, :, member * WIDTH:(member + 1) * WIDTH]
        diag_real, diag_imag = complex_dot(lower_real.T, lower_imag.T, upper_real, upper_imag)
        blocks.append(jnp.stack([diag_real, diag_imag]))
    correction = jnp.concatenate(blocks, axis=2)
    return offdiag, diag_inverse + correction
```

```python
import functools

import jax
import jax.numpy as jnp
from jax import lax
from jax.experimental import pallas as pl
from jax.experimental.pallas import tpu as pltpu
from jax.sharding import PartitionSpec as P

WIDTH = 512
VMEM_BUDGET = 48 * 2**20
MESH = pl.DeviceIdType.MESH


def row_of(position, half):
    upper = position // half
    level = position + upper * (2 * half - 1 - 2 * position)
    return 2 * level + upper


def position_of(row, half):
    level, upper = row // 2, row % 2
    return level + upper * (2 * half - 1 - 2 * level)


def gather_kernel(
    ring, pattern, inverse, panel, diag, off_out, diag_out,
    g, m, masked, coupled, pan, dg,
    load_sem, ring_send, ring_recv, pan_send, pan_recv,
    core_send, core_recv, side_send, side_recv, pass_send, pass_recv,
):
    half = ring // 2
    row, col = lax.axis_index("prow"), lax.axis_index("pcol")
    place = position_of(row, half)
    rows, part = inverse.shape[1], inverse.shape[2]
    fine, width = panel.shape[1], diag.shape[2]
    core_mate = col + 1 - 2 * (col % 2)
    side_mate = lax.rem(col + 2, 4)
    far_mate = lax.rem(core_mate + 2, 4)
    forward = row_of(lax.rem(place + 1, ring), half)
    backward = row_of(lax.rem(place + ring - 1, ring), half)
    targets = ((forward, col), (backward, col))

    def block_row(offset):
        return row_of(lax.rem(place + ring + offset, ring), half)

    def g_part(of_row, of_col):
        return g.at[
            :,
            pl.ds(pl.multiple_of(of_row * rows, rows), rows),
            pl.ds(pl.multiple_of(of_col * part, part), part),
        ]

    def m_part(of_row, of_col, first=0, count=2):
        start = pl.multiple_of(of_row * rows + of_col * fine, fine)
        return m.at[pl.ds(first, count), pl.ds(start, fine), :]

    def own_columns(of_col):
        return pan.at[:, :, pl.ds(pl.multiple_of(of_col * width, width), width)]

    load_panel = pltpu.make_async_copy(panel, pan, load_sem.at[0])
    load_g = pltpu.make_async_copy(inverse, g_part(row, col), load_sem.at[1])
    load_diag = pltpu.make_async_copy(diag, dg, load_sem.at[2])
    load_panel.start()
    load_g.start()

    barrier = pltpu.get_barrier_semaphore()
    partners = targets + ((row, core_mate), (row, side_mate), (row, far_mate))
    for partner in partners:
        pl.semaphore_signal(barrier, inc=1, device_id=partner, device_id_type=MESH)
    pl.semaphore_wait(barrier, len(partners))
    load_panel.wait()
    load_g.wait()

    started = []

    def send(src, dst, send_sem, recv_sem, target):
        copy = pltpu.make_async_remote_copy(
            src_ref=src, dst_ref=dst, send_sem=send_sem, recv_sem=recv_sem,
            device_id=target, device_id_type=MESH,
        )
        copy.start()
        started.append(copy)

    mates = (core_mate, side_mate, far_mate)
    sources = (col,) + mates

    def piece(offset, chunk):
        of_row = block_row(offset)
        if chunk == 0:
            return g_part(of_row, col)
        if chunk == 5:
            return m_part(of_row, side_mate, 0, 1)
        if chunk == 6:
            return m_part(of_row, side_mate, 1, 1)
        return m_part(of_row, sources[chunk - 1])

    full = (0, 1, 2, 3, 4)
    split = ((0, 1, 5), (2, 4, 6))

    def carried(d, hop):
        return full if hop < half else split[d]

    def hop_offset(d, hop):
        return -hop if d == 0 else hop

    def wait_recv(ref, sem):
        pltpu.make_async_copy(ref, ref, sem).wait()

    def ring_send_piece(d, hop, chunk, src=None):
        offset = hop_offset(d, hop - 1)
        ref = piece(offset, chunk)
        send(
            ref if src is None else src, ref,
            ring_send.at[d, hop - 1, chunk], ring_recv.at[d, hop - 1, chunk],
            targets[d],
        )

    def share_g(index, offset):
        ref = g_part(block_row(offset), col)
        send(ref, ref, core_send.at[index], core_recv.at[index], (row, core_mate))
        send(ref, ref, side_send.at[index], side_recv.at[index], (row, side_mate))

    def pass_g(index, offset):
        ref = g_part(block_row(offset), side_mate)
        wait_recv(ref, side_recv.at[index])
        send(ref, ref, pass_send.at[index], pass_recv.at[index], (row, core_mate))

    for d in (0, 1):
        ring_send_piece(d, 1, 0)
    for index in (1, 2, 0):
        send(
            own_columns(mates[index]), m_part(row, col),
            pan_send.at[index], pan_recv.at[index], (row, mates[index]),
        )
    for d in (0, 1):
        ring_send_piece(d, 1, 1, own_columns(col))
    share_g(0, 0)
    keep_own = pltpu.make_async_copy(own_columns(col), m_part(row, col), load_sem.at[3])
    keep_own.start()
    load_diag.start()
    for index in range(3):
        wait_recv(m_part(row, mates[index]), pan_recv.at[index])
        for d in (0, 1):
            ring_send_piece(d, 1, index + 2)
    pass_g(0, 0)
    blocks = [(0, 0)]
    for hop in range(1, half + 1):
        fresh = []
        order = full + (5, 6)
        for chunk in order:
            for d in (0, 1):
                if chunk not in carried(d, hop):
                    continue
                offset = hop_offset(d, hop)
                wait_recv(piece(offset, chunk), ring_recv.at[d, hop - 1, chunk])
                if hop + 1 < half:
                    ring_send_piece(d, hop + 1, chunk)
                elif hop + 1 == half:
                    if chunk in split[d]:
                        ring_send_piece(d, half, chunk)
                    elif chunk == 3:
                        ring_send_piece(d, half, 5 + d)
                if chunk == 0:
                    index = len(blocks)
                    blocks.append((index, offset))
                    fresh.append((index, offset))
                    share_g(index, offset)
            if chunk == 3 and hop < half:
                for index, offset in fresh:
                    pass_g(index, offset)
                fresh = []
        for index, offset in fresh:
            pass_g(index, offset)
    for index, offset in blocks:
        wait_recv(g_part(block_row(offset), core_mate), core_recv.at[index])
        wait_recv(g_part(block_row(offset), far_mate), pass_recv.at[index])
    keep_own.wait()

    super_index = col * width // WIDTH
    order_rows = g.shape[1]
    for block in range(order_rows // WIDTH):
        keep = pattern[block, super_index] > 0
        span = slice(block * WIDTH, (block + 1) * WIDTH)
        masked[:, span, :] = jnp.where(keep, m[:, span, :], jnp.zeros_like(m[:, span, :]))

    def dot(a, b, contract):
        return lax.dot_general(
            a, b, (((contract,), (0,)), ((), ())), preferred_element_type=jnp.float32
        )

    step = min(256, width)
    for start in range(0, width, step):
        cols = slice(start, start + step)
        real = dot(g[0], masked[0, :, cols], 1) - dot(g[1], masked[1, :, cols], 1)
        imag = dot(g[0], masked[1, :, cols], 1) + dot(g[1], masked[0, :, cols], 1)
        for block in range(order_rows // WIDTH):
            keep = (pattern[block, super_index] > 0).astype(jnp.float32)
            span = slice(block * WIDTH, (block + 1) * WIDTH)
            coupled[0, span, cols] = (real[span] * keep).astype(jnp.bfloat16)
            coupled[1, span, cols] = (imag[span] * keep).astype(jnp.bfloat16)
    off_out[...] = -coupled[:, pl.ds(pl.multiple_of(row * rows, rows), rows), :]
    load_diag.wait()
    for start in range(0, width, step):
        cols = slice(start, start + step)
        diag_out[0, :, cols] = dg[0, :, cols] + (
            dot(masked[0], coupled[0, :, cols], 0) - dot(masked[1], coupled[1, :, cols], 0)
        )
        diag_out[1, :, cols] = dg[1, :, cols] + (
            dot(masked[0], coupled[1, :, cols], 0) + dot(masked[1], coupled[0, :, cols], 0)
        )
    for copy in started:
        copy.wait_send()


def gathered(inverse_block, panel, pattern, diag_inverse):
    ring = lax.axis_size("prow")
    half = ring // 2
    rows = inverse_block.shape[1]
    order, width = rows * ring, diag_inverse.shape[2]
    dma = pltpu.SemaphoreType.DMA
    anywhere = pl.BlockSpec(memory_space=pl.ANY)
    whole = pl.BlockSpec(memory_space=pltpu.VMEM)
    return pl.pallas_call(
        functools.partial(gather_kernel, ring),
        out_shape=(
            jax.ShapeDtypeStruct((2, rows, width), jnp.bfloat16),
            jax.ShapeDtypeStruct(diag_inverse.shape, jnp.float32),
        ),
        in_specs=[pl.BlockSpec(memory_space=pltpu.SMEM), anywhere, anywhere, anywhere],
        out_specs=(whole, whole),
        scratch_shapes=[
            pltpu.VMEM((2, order, order), jnp.bfloat16),
            pltpu.VMEM((2, order, width), jnp.bfloat16),
            pltpu.VMEM((2, order, width), jnp.bfloat16),
            pltpu.VMEM((2, order, width), jnp.bfloat16),
            pltpu.VMEM(panel.shape, jnp.bfloat16),
            pltpu.VMEM(diag_inverse.shape, jnp.float32),
            dma((4,)),
            dma((2, half, 7)), dma((2, half, 7)),
            dma((3,)), dma((3,)),
            dma((ring,)), dma((ring,)),
            dma((ring,)), dma((ring,)),
            dma((ring,)), dma((ring,)),
        ],
        compiler_params=pltpu.CompilerParams(
            collective_id=0, has_side_effects=True, vmem_limit_bytes=VMEM_BUDGET
        ),
    )(pattern, inverse_block, panel, diag_inverse)


def fits(ring, col_count, inverse_block, panel, diag_inverse):
    order, width = inverse_block.shape[1] * ring, diag_inverse.shape[2]
    held = 4 * order * order + 8 * order * width + 16 * diag_inverse.shape[1] * width
    return (
        ring % 2 == 0 and ring >= 4 and col_count == 4 and width == WIDTH
        and panel.shape[1] % 16 == 0 and inverse_block.shape[2] % 128 == 0
        and order % WIDTH == 0 and held <= VMEM_BUDGET * 2 // 3
    )


def complex_product(left_real, left_imag, right_real, right_imag, contract):
    dims = (((contract,), (0,)), ((), ()))
    real_part = lax.dot_general(
        left_real, right_real, dims, preferred_element_type=jnp.float32
    ) - lax.dot_general(left_imag, right_imag, dims, preferred_element_type=jnp.float32)
    imag_part = lax.dot_general(
        left_real, right_imag, dims, preferred_element_type=jnp.float32
    ) + lax.dot_general(left_imag, right_real, dims, preferred_element_type=jnp.float32)
    return (real_part, imag_part)


def keep_table(pattern, row_start, row_count, col_start, col_count, block_width):
    row_ids = (row_start + jnp.arange(row_count, dtype=jnp.int32)) // block_width
    col_ids = (col_start + jnp.arange(col_count, dtype=jnp.int32)) // block_width
    row_select = (
        row_ids[:, None] == jnp.arange(pattern.shape[0], dtype=jnp.int32)[None, :]
    ).astype(jnp.float32)
    col_select = (
        col_ids[:, None] == jnp.arange(pattern.shape[1], dtype=jnp.int32)[None, :]
    ).astype(jnp.float32)
    pattern_value = pattern.astype(jnp.float32)
    row_pattern = jnp.dot(row_select, pattern_value, precision=lax.Precision.HIGHEST)
    return jnp.dot(row_pattern, col_select.T, precision=lax.Precision.HIGHEST)


def local(inverse_block, panel, pattern, diag_inverse):
    rows_dev = inverse_block.shape[1]
    block_span = inverse_block.shape[2]
    fine_rows = panel.shape[1]
    columns = panel.shape[2]
    if fits(lax.axis_size("prow"), lax.axis_size("pcol"), inverse_block, panel, diag_inverse):
        return gathered(inverse_block, panel, pattern, diag_inverse)
    row_index = lax.axis_index("prow")
    col_index = lax.axis_index("pcol")
    col_count = lax.axis_size("pcol")
    root_count = lax.axis_size("prow") // col_count
    fine_start = (row_index * col_count + col_index) * fine_rows
    keep_mask = keep_table(pattern, fine_start, fine_rows, 0, columns, WIDTH)
    masked = jnp.where(keep_mask[None] > 0.5, panel, jnp.zeros_like(panel))
    row_panel = lax.all_gather(masked, "pcol", axis=1, tiled=True)
    flipped = jnp.swapaxes(inverse_block, 1, 2)
    split_cols = flipped.reshape(2, root_count, col_count, fine_rows, rows_dev)
    received = lax.all_to_all(split_cols, "pcol", split_axis=2, concat_axis=1, tiled=True)
    regrouped = received.reshape(2, block_span, rows_dev)
    panel_piece = lax.all_gather(masked, "prow", axis=1, tiled=True)
    part_real, part_imag = complex_product(
        regrouped[0], regrouped[1], panel_piece[0], panel_piece[1], 0
    )
    stacked = jnp.stack([part_real, part_imag])
    summed = lax.psum_scatter(stacked, "pcol", scatter_dimension=2, tiled=True)
    local_cols = summed.shape[2]
    keep_local = keep_table(
        pattern, row_index * rows_dev, rows_dev, col_index * local_cols, local_cols, WIDTH
    )
    coupled = (summed * keep_local[None]).astype(jnp.bfloat16)
    offdiag = -coupled
    block_start = col_index * local_cols // WIDTH * WIDTH
    lower_panel = lax.dynamic_slice_in_dim(row_panel, block_start, WIDTH, 2)
    diag_real, diag_imag = complex_product(
        lower_panel[0], lower_panel[1], coupled[0], coupled[1], 0
    )
    shares = lax.psum_scatter(
        jnp.stack([diag_real, diag_imag]), "prow", scatter_dimension=1, tiled=True
    )
    correction = lax.all_gather(shares, "prow", axis=1, tiled=True)
    return (offdiag, diag_inverse + correction)


def solution(mesh):
    in_specs = (
        P(None, "prow", "pcol"),
        P(None, ("prow", "pcol"), None),
        P(),
        P(None, None, "pcol"),
    )
    out_specs = (P(None, "prow", "pcol"), P(None, None, "pcol"))
    return jax.shard_map(local, mesh=mesh, in_specs=in_specs, out_specs=out_specs, check_vma=False)
```

```python
import functools
import heapq

import jax
import jax.numpy as jnp
from jax import lax
from jax.experimental import pallas as pl
from jax.experimental.pallas import tpu as pltpu
from jax.sharding import PartitionSpec as P

WIDTH = 512
VMEM_BUDGET = 48 * 2**20
MESH = pl.DeviceIdType.MESH


def row_of(position, half):
    upper = position // half
    level = position + upper * (2 * half - 1 - 2 * position)
    return 2 * level + upper


def position_of(row, half):
    level, upper = row // 2, row % 2
    return level + upper * (2 * half - 1 - 2 * level)


def schedule(half, full, split, piece_time, link_delay, core_delay):
    free = {"ring0": 0.0, "ring1": 0.0, "side": 0.0, "core": 0.0}
    heap, order, serial = [], [], [0]

    def post(now, link, key, size=1.0):
        span = size * (piece_time if link != "core" else piece_time / 8)
        begin = max(now, free[link])
        free[link] = begin + span
        delay = core_delay if link == "core" else link_delay
        serial[0] += 1
        heapq.heappush(heap, (begin + span + delay, serial[0], key))

    def ring(now, d, hop, chunk):
        post(now, "ring%d" % d, ("ring", d, hop, chunk), 0.5 if chunk > 4 else 1.0)

    def share(now, index):
        post(now, "core", ("core", index))
        post(now, "side", ("side", index))

    for d in (0, 1):
        ring(0.0, d, 1, 0)
    post(0.0, "core", ("pan", 0))
    for index in (1, 2):
        post(0.0, "side", ("pan", index))
    for d in (0, 1):
        ring(0.0, d, 1, 1)
    share(0.0, (0, 0))
    while heap:
        now, _, key = heapq.heappop(heap)
        order.append(key)
        if key[0] == "pan":
            for d in (0, 1):
                ring(now, d, 1, key[1] + 2)
        elif key[0] == "side":
            post(now, "core", ("pass", key[1]))
        elif key[0] == "ring":
            _, d, hop, chunk = key
            for onward in carried_on(half, full, split, d, hop, chunk):
                ring(now, d, hop + 1, onward)
            if chunk == 0:
                share(now, (d, hop))
    return order


def carried_on(half, full, split, d, hop, chunk):
    if hop + 1 < half:
        return (chunk,)
    if hop + 1 > half:
        return ()
    if chunk in split[d]:
        return (chunk,)
    return (5 + d,) if chunk == 3 else ()


FULL = (0, 1, 2, 3, 4)
SPLIT = ((0, 1, 5), (2, 4, 6))


def gather_kernel(
    ring, pattern_hbm, inverse, panel, diag, masked, coupled, held,
    pattern, g, m, pan, acc, tail,
    load_sem, ring_send, ring_recv, pan_send, pan_recv,
    core_send, core_recv, side_send, side_recv, pass_send, pass_recv,
):
    half = ring // 2
    row, col = lax.axis_index("prow"), lax.axis_index("pcol")
    place = position_of(row, half)
    rows, part = inverse.shape[1], inverse.shape[2]
    fine, width = panel.shape[1], masked.shape[2]
    order_rows = g.shape[1]
    core_mate = col + 1 - 2 * (col % 2)
    side_mate = lax.rem(col + 2, 4)
    far_mate = lax.rem(core_mate + 2, 4)
    forward = row_of(lax.rem(place + 1, ring), half)
    backward = row_of(lax.rem(place + ring - 1, ring), half)
    targets = ((forward, col), (backward, col))
    mates = (core_mate, side_mate, far_mate)
    sources = (col,) + mates

    def block_row(offset):
        return row_of(lax.rem(place + ring + offset, ring), half)

    def g_part(of_row, of_col):
        return g.at[
            :,
            pl.ds(pl.multiple_of(of_row * rows, rows), rows),
            pl.ds(pl.multiple_of(of_col * part, part), part),
        ]

    def m_part(of_row, of_col, first=0, count=2):
        start = pl.multiple_of(of_row * rows + of_col * fine, fine)
        return m.at[pl.ds(first, count), pl.ds(start, fine), :]

    def own_columns(of_col):
        return pan.at[:, :, pl.ds(pl.multiple_of(of_col * width, width), width)]

    load_panel = pltpu.make_async_copy(panel, pan, load_sem.at[0])
    load_g = pltpu.make_async_copy(inverse, g_part(row, col), load_sem.at[1])
    load_pattern = pltpu.make_async_copy(pattern_hbm, pattern, load_sem.at[2])
    load_g.start()
    load_panel.start()
    load_pattern.start()

    barrier = pltpu.get_barrier_semaphore()
    partners = targets + tuple((row, mate) for mate in mates)
    for partner in partners:
        pl.semaphore_signal(barrier, inc=1, device_id=partner, device_id_type=MESH)
    pl.semaphore_wait(barrier, len(partners))

    started = []

    def send(src, dst, send_sem, recv_sem, target):
        copy = pltpu.make_async_remote_copy(
            src_ref=src, dst_ref=dst, send_sem=send_sem, recv_sem=recv_sem,
            device_id=target, device_id_type=MESH,
        )
        copy.start()
        started.append(copy)

    def piece(offset, chunk):
        of_row = block_row(offset)
        if chunk == 0:
            return g_part(of_row, col)
        if chunk > 4:
            return m_part(of_row, side_mate, chunk - 5, 1)
        return m_part(of_row, sources[chunk - 1])

    def offset_of(key):
        return -key[1] if key[0] == 0 else key[1]

    def slot(key):
        return key[0] * half + key[1]

    def wait_recv(ref, sem):
        pltpu.make_async_copy(ref, ref, sem).wait()

    def ring_on(d, hop, chunk, src=None):
        ref = piece(offset_of((d, hop - 1)), chunk)
        send(
            ref if src is None else src, ref,
            ring_send.at[d, hop - 1, chunk], ring_recv.at[d, hop - 1, chunk], targets[d],
        )

    def share_g(key):
        ref, at = g_part(block_row(offset_of(key)), col), slot(key)
        send(ref, ref, core_send.at[at], core_recv.at[at], (row, core_mate))
        send(ref, ref, side_send.at[at], side_recv.at[at], (row, side_mate))

    def handle(key):
        if key[0] == "pan":
            wait_recv(m_part(row, mates[key[1]]), pan_recv.at[key[1]])
            for d in (0, 1):
                ring_on(d, 1, key[1] + 2)
        elif key[0] == "side":
            ref, at = g_part(block_row(offset_of(key[1])), side_mate), slot(key[1])
            wait_recv(ref, side_recv.at[at])
            send(ref, ref, pass_send.at[at], pass_recv.at[at], (row, core_mate))
        elif key[0] == "core":
            wait_recv(g_part(block_row(offset_of(key[1])), core_mate), core_recv.at[slot(key[1])])
        elif key[0] == "pass":
            wait_recv(g_part(block_row(offset_of(key[1])), far_mate), pass_recv.at[slot(key[1])])
        else:
            _, d, hop, chunk = key
            wait_recv(piece(offset_of((d, hop)), chunk), ring_recv.at[d, hop - 1, chunk])
            for onward in carried_on(half, FULL, SPLIT, d, hop, chunk):
                ring_on(d, hop + 1, onward)
            if chunk == 0:
                share_g((d, hop))

    load_g.wait()
    for d in (0, 1):
        ring_on(d, 1, 0)
    load_panel.wait()
    for index in (1, 2, 0):
        send(
            own_columns(mates[index]), m_part(row, col),
            pan_send.at[index], pan_recv.at[index], (row, mates[index]),
        )
    for d in (0, 1):
        ring_on(d, 1, 1, own_columns(col))
    share_g((0, 0))
    keep_own = pltpu.make_async_copy(own_columns(col), m_part(row, col), load_sem.at[3])
    keep_own.start()
    load_diag = pltpu.make_async_copy(diag, held, load_sem.at[4])
    load_diag.start()

    keys = schedule(half, FULL, SPLIT, 0.78, 1.65, 0.9)
    last = [k for k in keys if k[0] == "ring" and k[2] == half and k[3] > 0]
    inert = [k for k in keys if k[0] in ("core", "pass")]
    for key in keys:
        if key not in last and key not in inert:
            handle(key)
    keep_own.wait()
    load_diag.wait()
    load_pattern.wait()

    super_index = col * width // WIDTH

    def rows_of(of_row):
        return pl.ds(pl.multiple_of(of_row * rows, rows), rows)

    def masked_rows(of_row):
        keep = pattern[of_row * rows // WIDTH, super_index] > 0
        values = m[:, rows_of(of_row), :]
        return jnp.where(keep, values, jnp.zeros_like(values))

    far_row = block_row(half)
    for offset in range(1 - half, half):
        of_row = block_row(offset)
        masked[:, rows_of(of_row), :] = masked_rows(of_row)
    masked[:, rows_of(far_row), :] = jnp.zeros((2, rows, width), masked.dtype)
    for key in inert:
        handle(key)

    step = min(256, width)
    for start in range(0, width, step):
        cols = slice(start, start + step)
        acc[0, :, cols] = dot(g[0], masked[0, :, cols], 1) - dot(g[1], masked[1, :, cols], 1)
        acc[1, :, cols] = dot(g[0], masked[1, :, cols], 1) + dot(g[1], masked[0, :, cols], 1)

    for key in last:
        handle(key)
    span = tail.shape[1]
    tail[...] = jnp.zeros_like(tail)
    far_values = masked_rows(far_row)
    masked[:, rows_of(far_row), :] = far_values
    tail[:, pl.ds(pl.multiple_of(lax.rem(far_row * rows, span), rows), rows), :] = far_values
    lanes = pl.ds(pl.multiple_of(far_row * rows // span * span, span), span)
    for start in range(0, width, step):
        cols = slice(start, start + step)
        real = acc[0, :, cols] + (
            dot(g[0, :, lanes], tail[0, :, cols], 1) - dot(g[1, :, lanes], tail[1, :, cols], 1)
        )
        imag = acc[1, :, cols] + (
            dot(g[0, :, lanes], tail[1, :, cols], 1) + dot(g[1, :, lanes], tail[0, :, cols], 1)
        )
        for block in range(order_rows // WIDTH):
            keep = (pattern[block, super_index] > 0).astype(jnp.float32)
            band = slice(block * WIDTH, (block + 1) * WIDTH)
            coupled[0, band, cols] = (real[band] * keep).astype(jnp.bfloat16)
            coupled[1, band, cols] = (imag[band] * keep).astype(jnp.bfloat16)
    for copy in started:
        copy.wait_send()


def dot(a, b, contract):
    return lax.dot_general(
        a, b, (((contract,), (0,)), ((), ())), preferred_element_type=jnp.float32
    )


def correct_kernel(masked, coupled, held, off_out, diag_out, off, total, save_sem):
    rows, height = off.shape[1], total.shape[1]
    row = lax.axis_index("prow")
    off[...] = -coupled[:, pl.ds(pl.multiple_of(row * rows, rows), rows), :]
    saves = [pltpu.make_async_copy(off, off_out, save_sem.at[0])]
    saves[0].start()
    step = min(256, height)
    for start in range(0, height, step):
        span = slice(start, start + step)
        for which in (0, 1):
            first = dot(masked[0, :, span], coupled[which], 0)
            second = dot(masked[1, :, span], coupled[1 - which], 0)
            total[which, span, :] = held[which, span, :] + (
                first - second if which == 0 else first + second
            )
            save = pltpu.make_async_copy(
                total.at[which, span, :], diag_out.at[which, span, :], save_sem.at[len(saves)]
            )
            save.start()
            saves.append(save)
    for save in saves:
        save.wait()


def in_hbm(array):
    return pltpu.with_memory_space_constraint(array, pltpu.HBM)


def gathered(inverse_block, panel, pattern, diag_inverse):
    ring = lax.axis_size("prow")
    half = ring // 2
    rows = inverse_block.shape[1]
    order, width, height = rows * ring, diag_inverse.shape[2], diag_inverse.shape[1]
    dma = pltpu.SemaphoreType.DMA
    anywhere = pl.BlockSpec(memory_space=pl.ANY)
    whole = pl.BlockSpec(memory_space=pltpu.VMEM)
    tall = jax.ShapeDtypeStruct((2, order, width), jnp.bfloat16)
    masked, coupled, held = pl.pallas_call(
        functools.partial(gather_kernel, ring),
        out_shape=(tall, tall, jax.ShapeDtypeStruct(diag_inverse.shape, jnp.float32)),
        in_specs=[anywhere] * 4,
        out_specs=(whole,) * 3,
        scratch_shapes=[
            pltpu.SMEM(pattern.shape, jnp.int32),
            pltpu.VMEM((2, order, order), jnp.bfloat16),
            pltpu.VMEM((2, order, width), jnp.bfloat16),
            pltpu.VMEM(panel.shape, jnp.bfloat16),
            pltpu.VMEM((2, order, width), jnp.float32),
            pltpu.VMEM((2, max(rows, 128), width), jnp.bfloat16),
            dma((5,)),
            dma((2, half, 7)), dma((2, half, 7)),
            dma((3,)), dma((3,)),
            dma((ring + 1,)), dma((ring + 1,)),
            dma((ring + 1,)), dma((ring + 1,)),
            dma((ring + 1,)), dma((ring + 1,)),
        ],
        compiler_params=pltpu.CompilerParams(
            collective_id=0, has_side_effects=True, vmem_limit_bytes=VMEM_BUDGET
        ),
    )(in_hbm(pattern), in_hbm(inverse_block), in_hbm(panel), in_hbm(diag_inverse))
    return pl.pallas_call(
        correct_kernel,
        out_shape=(
            jax.ShapeDtypeStruct((2, rows, width), jnp.bfloat16),
            jax.ShapeDtypeStruct(diag_inverse.shape, jnp.float32),
        ),
        in_specs=[whole] * 3,
        out_specs=(anywhere, anywhere),
        scratch_shapes=[
            pltpu.VMEM((2, rows, width), jnp.bfloat16),
            pltpu.VMEM(diag_inverse.shape, jnp.float32),
            dma((2 * pl.cdiv(height, 256) + 1,)),
        ],
        compiler_params=pltpu.CompilerParams(vmem_limit_bytes=VMEM_BUDGET),
    )(masked, coupled, held)


def fits(ring, col_count, inverse_block, panel, diag_inverse):
    rows, width = inverse_block.shape[1], diag_inverse.shape[2]
    order = rows * ring
    held = 4 * order * order + 8 * order * width + 16 * diag_inverse.shape[1] * width
    return (
        ring % 2 == 0 and ring >= 4 and col_count == 4 and width == WIDTH
        and panel.shape[1] % 16 == 0 and inverse_block.shape[2] % 128 == 0
        and order % WIDTH == 0 and max(rows, 128) % rows == 0 and rows % 16 == 0
        and WIDTH % rows == 0 and held <= VMEM_BUDGET * 2 // 3
    )


def complex_product(left_real, left_imag, right_real, right_imag, contract):
    dims = (((contract,), (0,)), ((), ()))
    real_part = lax.dot_general(
        left_real, right_real, dims, preferred_element_type=jnp.float32
    ) - lax.dot_general(left_imag, right_imag, dims, preferred_element_type=jnp.float32)
    imag_part = lax.dot_general(
        left_real, right_imag, dims, preferred_element_type=jnp.float32
    ) + lax.dot_general(left_imag, right_real, dims, preferred_element_type=jnp.float32)
    return (real_part, imag_part)


def keep_table(pattern, row_start, row_count, col_start, col_count, block_width):
    row_ids = (row_start + jnp.arange(row_count, dtype=jnp.int32)) // block_width
    col_ids = (col_start + jnp.arange(col_count, dtype=jnp.int32)) // block_width
    row_select = (
        row_ids[:, None] == jnp.arange(pattern.shape[0], dtype=jnp.int32)[None, :]
    ).astype(jnp.float32)
    col_select = (
        col_ids[:, None] == jnp.arange(pattern.shape[1], dtype=jnp.int32)[None, :]
    ).astype(jnp.float32)
    pattern_value = pattern.astype(jnp.float32)
    row_pattern = jnp.dot(row_select, pattern_value, precision=lax.Precision.HIGHEST)
    return jnp.dot(row_pattern, col_select.T, precision=lax.Precision.HIGHEST)


def local(inverse_block, panel, pattern, diag_inverse):
    rows_dev = inverse_block.shape[1]
    block_span = inverse_block.shape[2]
    fine_rows = panel.shape[1]
    columns = panel.shape[2]
    if fits(lax.axis_size("prow"), lax.axis_size("pcol"), inverse_block, panel, diag_inverse):
        return gathered(inverse_block, panel, pattern, diag_inverse)
    row_index = lax.axis_index("prow")
    col_index = lax.axis_index("pcol")
    col_count = lax.axis_size("pcol")
    root_count = lax.axis_size("prow") // col_count
    fine_start = (row_index * col_count + col_index) * fine_rows
    keep_mask = keep_table(pattern, fine_start, fine_rows, 0, columns, WIDTH)
    masked = jnp.where(keep_mask[None] > 0.5, panel, jnp.zeros_like(panel))
    row_panel = lax.all_gather(masked, "pcol", axis=1, tiled=True)
    flipped = jnp.swapaxes(inverse_block, 1, 2)
    split_cols = flipped.reshape(2, root_count, col_count, fine_rows, rows_dev)
    received = lax.all_to_all(split_cols, "pcol", split_axis=2, concat_axis=1, tiled=True)
    regrouped = received.reshape(2, block_span, rows_dev)
    panel_piece = lax.all_gather(masked, "prow", axis=1, tiled=True)
    part_real, part_imag = complex_product(
        regrouped[0], regrouped[1], panel_piece[0], panel_piece[1], 0
    )
    stacked = jnp.stack([part_real, part_imag])
    summed = lax.psum_scatter(stacked, "pcol", scatter_dimension=2, tiled=True)
    local_cols = summed.shape[2]
    keep_local = keep_table(
        pattern, row_index * rows_dev, rows_dev, col_index * local_cols, local_cols, WIDTH
    )
    coupled = (summed * keep_local[None]).astype(jnp.bfloat16)
    offdiag = -coupled
    block_start = col_index * local_cols // WIDTH * WIDTH
    lower_panel = lax.dynamic_slice_in_dim(row_panel, block_start, WIDTH, 2)
    diag_real, diag_imag = complex_product(
        lower_panel[0], lower_panel[1], coupled[0], coupled[1], 0
    )
    shares = lax.psum_scatter(
        jnp.stack([diag_real, diag_imag]), "prow", scatter_dimension=1, tiled=True
    )
    correction = lax.all_gather(shares, "prow", axis=1, tiled=True)
    return (offdiag, diag_inverse + correction)


def solution(mesh):
    in_specs = (
        P(None, "prow", "pcol"),
        P(None, ("prow", "pcol"), None),
        P(),
        P(None, None, "pcol"),
    )
    out_specs = (P(None, "prow", "pcol"), P(None, None, "pcol"))
    return jax.shard_map(local, mesh=mesh, in_specs=in_specs, out_specs=out_specs, check_vma=False)
```

```python
import functools
import heapq

import jax
import jax.numpy as jnp
from jax import lax
from jax.experimental import pallas as pl
from jax.experimental.pallas import tpu as pltpu
from jax.sharding import PartitionSpec as P

WIDTH = 512
VMEM_BUDGET = 48 * 2**20
MESH = pl.DeviceIdType.MESH


def row_of(position, half):
    upper = position // half
    level = position + upper * (2 * half - 1 - 2 * position)
    return 2 * level + upper


def position_of(row, half):
    level, upper = row // 2, row % 2
    return level + upper * (2 * half - 1 - 2 * level)


def schedule(half, piece_time, link_delay, core_delay, backlog):
    free = {"ring0": 0.0, "ring1": 0.0, "side": 0.0, "core": 0.0}
    heap, order, serial, held = [], [], [0], ([], [])

    def post(now, link, key, size=1.0):
        span = size * (piece_time if link != "core" else piece_time / 8)
        begin = max(now, free[link])
        free[link] = begin + span
        delay = core_delay if link == "core" else link_delay
        serial[0] += 1
        heapq.heappush(heap, (begin + span + delay, serial[0], key))

    def ring(now, d, hop, chunk):
        post(now, "ring%d" % d, ("ring", d, hop, chunk), 0.5 if chunk > 4 else 1.0)
        order.append(("send", d, hop, chunk))

    def share(now, index):
        post(now, "core", ("core", index))
        post(now, "side", ("side", index))

    def release(now, limit):
        for d in (0, 1):
            while held[d] and free["ring%d" % d] - now < limit:
                ring(now, d, *held[d].pop(0))

    for d in (0, 1):
        ring(0.0, d, 1, 0)
    post(0.0, "core", ("pan", 0))
    for index in (1, 2):
        post(0.0, "side", ("pan", index))
    for d in (0, 1):
        ring(0.0, d, 1, 1)
    share(0.0, (0, 0))
    order.clear()
    while heap or held[0] or held[1]:
        if not heap:
            release(0.0, float("inf"))
        now, _, key = heapq.heappop(heap)
        order.append(key)
        if key[0] == "pan":
            for d in (0, 1):
                held[d].append((1, key[1] + 2))
        elif key[0] == "side":
            post(now, "core", ("pass", key[1]))
        elif key[0] == "ring":
            _, d, hop, chunk = key
            for onward in carried_on(half, FULL, SPLIT, d, hop, chunk):
                if onward == 0:
                    ring(now, d, hop + 1, 0)
                else:
                    held[d].append((hop + 1, onward))
            if chunk == 0:
                share(now, (d, hop))
        release(now, backlog)
    return order


def carried_on(half, full, split, d, hop, chunk):
    if hop + 1 < half:
        return (chunk,)
    if hop + 1 > half:
        return ()
    if chunk in split[d]:
        return (chunk,)
    return (5 + d,) if chunk == 3 else ()


FULL = (0, 1, 2, 3, 4)
SPLIT = ((0, 1, 5), (2, 4, 6))


def gather_kernel(
    ring, pattern_hbm, inverse, panel, diag, masked, coupled, held,
    pattern, g, m, pan, acc, tail,
    load_sem, ring_send, ring_recv, pan_send, pan_recv,
    core_send, core_recv, side_send, side_recv, pass_send, pass_recv,
):
    half = ring // 2
    row, col = lax.axis_index("prow"), lax.axis_index("pcol")
    place = position_of(row, half)
    rows, part = inverse.shape[1], inverse.shape[2]
    fine, width = panel.shape[1], masked.shape[2]
    order_rows = g.shape[1]
    core_mate = col + 1 - 2 * (col % 2)
    side_mate = lax.rem(col + 2, 4)
    far_mate = lax.rem(core_mate + 2, 4)
    forward = row_of(lax.rem(place + 1, ring), half)
    backward = row_of(lax.rem(place + ring - 1, ring), half)
    targets = ((forward, col), (backward, col))
    mates = (core_mate, side_mate, far_mate)
    sources = (col,) + mates

    def block_row(offset):
        return row_of(lax.rem(place + ring + offset, ring), half)

    def g_part(of_row, of_col):
        return g.at[
            :,
            pl.ds(pl.multiple_of(of_row * rows, rows), rows),
            pl.ds(pl.multiple_of(of_col * part, part), part),
        ]

    def m_part(of_row, of_col, first=0, count=2):
        start = pl.multiple_of(of_row * rows + of_col * fine, fine)
        return m.at[pl.ds(first, count), pl.ds(start, fine), :]

    def own_columns(of_col):
        return pan.at[:, :, pl.ds(pl.multiple_of(of_col * width, width), width)]

    load_panel = pltpu.make_async_copy(panel, pan, load_sem.at[0])
    load_g = pltpu.make_async_copy(inverse, g_part(row, col), load_sem.at[1])
    load_pattern = pltpu.make_async_copy(pattern_hbm, pattern, load_sem.at[2])
    load_g.start()
    load_panel.start()
    load_pattern.start()

    barrier = pltpu.get_barrier_semaphore()
    partners = targets + tuple((row, mate) for mate in mates)
    for partner in partners:
        pl.semaphore_signal(barrier, inc=1, device_id=partner, device_id_type=MESH)
    pl.semaphore_wait(barrier, len(partners))

    started = []

    def send(src, dst, send_sem, recv_sem, target):
        copy = pltpu.make_async_remote_copy(
            src_ref=src, dst_ref=dst, send_sem=send_sem, recv_sem=recv_sem,
            device_id=target, device_id_type=MESH,
        )
        copy.start()
        started.append(copy)

    def piece(offset, chunk):
        of_row = block_row(offset)
        if chunk == 0:
            return g_part(of_row, col)
        if chunk > 4:
            return m_part(of_row, side_mate, chunk - 5, 1)
        return m_part(of_row, sources[chunk - 1])

    def offset_of(key):
        return -key[1] if key[0] == 0 else key[1]

    def slot(key):
        return key[0] * half + key[1]

    def wait_recv(ref, sem):
        pltpu.make_async_copy(ref, ref, sem).wait()

    def ring_on(d, hop, chunk, src=None):
        ref = piece(offset_of((d, hop - 1)), chunk)
        send(
            ref if src is None else src, ref,
            ring_send.at[d, hop - 1, chunk], ring_recv.at[d, hop - 1, chunk], targets[d],
        )

    def share_g(key):
        ref, at = g_part(block_row(offset_of(key)), col), slot(key)
        send(ref, ref, core_send.at[at], core_recv.at[at], (row, core_mate))
        send(ref, ref, side_send.at[at], side_recv.at[at], (row, side_mate))

    def handle(key):
        if key[0] == "pan":
            wait_recv(m_part(row, mates[key[1]]), pan_recv.at[key[1]])
        elif key[0] == "send":
            ring_on(*key[1:])
        elif key[0] == "side":
            ref, at = g_part(block_row(offset_of(key[1])), side_mate), slot(key[1])
            wait_recv(ref, side_recv.at[at])
            send(ref, ref, pass_send.at[at], pass_recv.at[at], (row, core_mate))
        elif key[0] == "core":
            wait_recv(g_part(block_row(offset_of(key[1])), core_mate), core_recv.at[slot(key[1])])
        elif key[0] == "pass":
            wait_recv(g_part(block_row(offset_of(key[1])), far_mate), pass_recv.at[slot(key[1])])
        else:
            _, d, hop, chunk = key
            wait_recv(piece(offset_of((d, hop)), chunk), ring_recv.at[d, hop - 1, chunk])
            if chunk == 0:
                share_g((d, hop))

    load_g.wait()
    for d in (0, 1):
        ring_on(d, 1, 0)
    load_panel.wait()
    for index in (1, 2, 0):
        send(
            own_columns(mates[index]), m_part(row, col),
            pan_send.at[index], pan_recv.at[index], (row, mates[index]),
        )
    for d in (0, 1):
        ring_on(d, 1, 1, own_columns(col))
    share_g((0, 0))
    keep_own = pltpu.make_async_copy(own_columns(col), m_part(row, col), load_sem.at[3])
    keep_own.start()
    load_diag = pltpu.make_async_copy(diag, held, load_sem.at[4])
    load_diag.start()

    keys = schedule(half, 0.78, 1.65, 0.9, 1.0)
    last = [k for k in keys if k[0] == "ring" and k[2] == half and k[3] > 0]
    inert = [k for k in keys if k[0] in ("core", "pass")]
    for key in keys:
        if key not in last and key not in inert:
            handle(key)
    keep_own.wait()
    load_diag.wait()
    load_pattern.wait()

    super_index = col * width // WIDTH

    def rows_of(of_row):
        return pl.ds(pl.multiple_of(of_row * rows, rows), rows)

    def masked_rows(of_row):
        keep = pattern[of_row * rows // WIDTH, super_index] > 0
        values = m[:, rows_of(of_row), :]
        return jnp.where(keep, values, jnp.zeros_like(values))

    far_row = block_row(half)
    for offset in range(1 - half, half):
        of_row = block_row(offset)
        masked[:, rows_of(of_row), :] = masked_rows(of_row)
    masked[:, rows_of(far_row), :] = jnp.zeros((2, rows, width), masked.dtype)
    for key in inert:
        handle(key)

    step = min(256, width)
    for start in range(0, width, step):
        cols = slice(start, start + step)
        acc[0, :, cols] = dot(g[0], masked[0, :, cols], 1) - dot(g[1], masked[1, :, cols], 1)
        acc[1, :, cols] = dot(g[0], masked[1, :, cols], 1) + dot(g[1], masked[0, :, cols], 1)

    for key in last:
        handle(key)
    span = tail.shape[1]
    tail[...] = jnp.zeros_like(tail)
    far_values = masked_rows(far_row)
    masked[:, rows_of(far_row), :] = far_values
    tail[:, pl.ds(pl.multiple_of(lax.rem(far_row * rows, span), rows), rows), :] = far_values
    lanes = pl.ds(pl.multiple_of(far_row * rows // span * span, span), span)
    for start in range(0, width, step):
        cols = slice(start, start + step)
        real = acc[0, :, cols] + (
            dot(g[0, :, lanes], tail[0, :, cols], 1) - dot(g[1, :, lanes], tail[1, :, cols], 1)
        )
        imag = acc[1, :, cols] + (
            dot(g[0, :, lanes], tail[1, :, cols], 1) + dot(g[1, :, lanes], tail[0, :, cols], 1)
        )
        for block in range(order_rows // WIDTH):
            keep = (pattern[block, super_index] > 0).astype(jnp.float32)
            band = slice(block * WIDTH, (block + 1) * WIDTH)
            coupled[0, band, cols] = (real[band] * keep).astype(jnp.bfloat16)
            coupled[1, band, cols] = (imag[band] * keep).astype(jnp.bfloat16)
    for copy in started:
        copy.wait_send()


def dot(a, b, contract):
    return lax.dot_general(
        a, b, (((contract,), (0,)), ((), ())), preferred_element_type=jnp.float32
    )


def correct_kernel(masked, coupled, held, off_out, diag_out, off, total, save_sem):
    rows, height = off.shape[1], total.shape[1]
    row = lax.axis_index("prow")
    off[...] = -coupled[:, pl.ds(pl.multiple_of(row * rows, rows), rows), :]
    saves = [pltpu.make_async_copy(off, off_out, save_sem.at[0])]
    saves[0].start()
    step = min(256, height)
    for start in range(0, height, step):
        span = slice(start, start + step)
        for which in (0, 1):
            first = dot(masked[0, :, span], coupled[which], 0)
            second = dot(masked[1, :, span], coupled[1 - which], 0)
            total[which, span, :] = held[which, span, :] + (
                first - second if which == 0 else first + second
            )
            save = pltpu.make_async_copy(
                total.at[which, span, :], diag_out.at[which, span, :], save_sem.at[len(saves)]
            )
            save.start()
            saves.append(save)
    for save in saves:
        save.wait()


def in_hbm(array):
    return pltpu.with_memory_space_constraint(array, pltpu.HBM)


def gathered(inverse_block, panel, pattern, diag_inverse):
    ring = lax.axis_size("prow")
    half = ring // 2
    rows = inverse_block.shape[1]
    order, width, height = rows * ring, diag_inverse.shape[2], diag_inverse.shape[1]
    dma = pltpu.SemaphoreType.DMA
    anywhere = pl.BlockSpec(memory_space=pl.ANY)
    whole = pl.BlockSpec(memory_space=pltpu.VMEM)
    tall = jax.ShapeDtypeStruct((2, order, width), jnp.bfloat16)
    masked, coupled, held = pl.pallas_call(
        functools.partial(gather_kernel, ring),
        out_shape=(tall, tall, jax.ShapeDtypeStruct(diag_inverse.shape, jnp.float32)),
        in_specs=[anywhere] * 4,
        out_specs=(whole,) * 3,
        scratch_shapes=[
            pltpu.SMEM(pattern.shape, jnp.int32),
            pltpu.VMEM((2, order, order), jnp.bfloat16),
            pltpu.VMEM((2, order, width), jnp.bfloat16),
            pltpu.VMEM(panel.shape, jnp.bfloat16),
            pltpu.VMEM((2, order, width), jnp.float32),
            pltpu.VMEM((2, max(rows, 128), width), jnp.bfloat16),
            dma((5,)),
            dma((2, half, 7)), dma((2, half, 7)),
            dma((3,)), dma((3,)),
            dma((ring + 1,)), dma((ring + 1,)),
            dma((ring + 1,)), dma((ring + 1,)),
            dma((ring + 1,)), dma((ring + 1,)),
        ],
        compiler_params=pltpu.CompilerParams(
            collective_id=0, has_side_effects=True, vmem_limit_bytes=VMEM_BUDGET
        ),
    )(in_hbm(pattern), in_hbm(inverse_block), in_hbm(panel), in_hbm(diag_inverse))
    return pl.pallas_call(
        correct_kernel,
        out_shape=(
            jax.ShapeDtypeStruct((2, rows, width), jnp.bfloat16),
            jax.ShapeDtypeStruct(diag_inverse.shape, jnp.float32),
        ),
        in_specs=[whole] * 3,
        out_specs=(anywhere, anywhere),
        scratch_shapes=[
            pltpu.VMEM((2, rows, width), jnp.bfloat16),
            pltpu.VMEM(diag_inverse.shape, jnp.float32),
            dma((2 * pl.cdiv(height, 256) + 1,)),
        ],
        compiler_params=pltpu.CompilerParams(vmem_limit_bytes=VMEM_BUDGET),
    )(masked, coupled, held)


def fits(ring, col_count, inverse_block, panel, diag_inverse):
    rows, width = inverse_block.shape[1], diag_inverse.shape[2]
    order = rows * ring
    held = 4 * order * order + 8 * order * width + 16 * diag_inverse.shape[1] * width
    return (
        ring % 2 == 0 and ring >= 4 and col_count == 4 and width == WIDTH
        and panel.shape[1] % 16 == 0 and inverse_block.shape[2] % 128 == 0
        and order % WIDTH == 0 and max(rows, 128) % rows == 0 and rows % 16 == 0
        and WIDTH % rows == 0 and held <= VMEM_BUDGET * 2 // 3
    )


def complex_product(left_real, left_imag, right_real, right_imag, contract):
    dims = (((contract,), (0,)), ((), ()))
    real_part = lax.dot_general(
        left_real, right_real, dims, preferred_element_type=jnp.float32
    ) - lax.dot_general(left_imag, right_imag, dims, preferred_element_type=jnp.float32)
    imag_part = lax.dot_general(
        left_real, right_imag, dims, preferred_element_type=jnp.float32
    ) + lax.dot_general(left_imag, right_real, dims, preferred_element_type=jnp.float32)
    return (real_part, imag_part)


def keep_table(pattern, row_start, row_count, col_start, col_count, block_width):
    row_ids = (row_start + jnp.arange(row_count, dtype=jnp.int32)) // block_width
    col_ids = (col_start + jnp.arange(col_count, dtype=jnp.int32)) // block_width
    row_select = (
        row_ids[:, None] == jnp.arange(pattern.shape[0], dtype=jnp.int32)[None, :]
    ).astype(jnp.float32)
    col_select = (
        col_ids[:, None] == jnp.arange(pattern.shape[1], dtype=jnp.int32)[None, :]
    ).astype(jnp.float32)
    pattern_value = pattern.astype(jnp.float32)
    row_pattern = jnp.dot(row_select, pattern_value, precision=lax.Precision.HIGHEST)
    return jnp.dot(row_pattern, col_select.T, precision=lax.Precision.HIGHEST)


def local(inverse_block, panel, pattern, diag_inverse):
    rows_dev = inverse_block.shape[1]
    block_span = inverse_block.shape[2]
    fine_rows = panel.shape[1]
    columns = panel.shape[2]
    if fits(lax.axis_size("prow"), lax.axis_size("pcol"), inverse_block, panel, diag_inverse):
        return gathered(inverse_block, panel, pattern, diag_inverse)
    row_index = lax.axis_index("prow")
    col_index = lax.axis_index("pcol")
    col_count = lax.axis_size("pcol")
    root_count = lax.axis_size("prow") // col_count
    fine_start = (row_index * col_count + col_index) * fine_rows
    keep_mask = keep_table(pattern, fine_start, fine_rows, 0, columns, WIDTH)
    masked = jnp.where(keep_mask[None] > 0.5, panel, jnp.zeros_like(panel))
    row_panel = lax.all_gather(masked, "pcol", axis=1, tiled=True)
    flipped = jnp.swapaxes(inverse_block, 1, 2)
    split_cols = flipped.reshape(2, root_count, col_count, fine_rows, rows_dev)
    received = lax.all_to_all(split_cols, "pcol", split_axis=2, concat_axis=1, tiled=True)
    regrouped = received.reshape(2, block_span, rows_dev)
    panel_piece = lax.all_gather(masked, "prow", axis=1, tiled=True)
    part_real, part_imag = complex_product(
        regrouped[0], regrouped[1], panel_piece[0], panel_piece[1], 0
    )
    stacked = jnp.stack([part_real, part_imag])
    summed = lax.psum_scatter(stacked, "pcol", scatter_dimension=2, tiled=True)
    local_cols = summed.shape[2]
    keep_local = keep_table(
        pattern, row_index * rows_dev, rows_dev, col_index * local_cols, local_cols, WIDTH
    )
    coupled = (summed * keep_local[None]).astype(jnp.bfloat16)
    offdiag = -coupled
    block_start = col_index * local_cols // WIDTH * WIDTH
    lower_panel = lax.dynamic_slice_in_dim(row_panel, block_start, WIDTH, 2)
    diag_real, diag_imag = complex_product(
        lower_panel[0], lower_panel[1], coupled[0], coupled[1], 0
    )
    shares = lax.psum_scatter(
        jnp.stack([diag_real, diag_imag]), "prow", scatter_dimension=1, tiled=True
    )
    correction = lax.all_gather(shares, "prow", axis=1, tiled=True)
    return (offdiag, diag_inverse + correction)


def solution(mesh):
    in_specs = (
        P(None, "prow", "pcol"),
        P(None, ("prow", "pcol"), None),
        P(),
        P(None, None, "pcol"),
    )
    out_specs = (P(None, "prow", "pcol"), P(None, None, "pcol"))
    return jax.shard_map(local, mesh=mesh, in_specs=in_specs, out_specs=out_specs, check_vma=False)
```

```python
import functools
import heapq

import jax
import jax.numpy as jnp
from jax import lax
from jax.experimental import pallas as pl
from jax.experimental.pallas import tpu as pltpu
from jax.sharding import PartitionSpec as P

WIDTH = 512
VMEM_BUDGET = 48 * 2**20
MESH = pl.DeviceIdType.MESH


def row_of(position, half):
    upper = position // half
    level = position + upper * (2 * half - 1 - 2 * position)
    return 2 * level + upper


def position_of(row, half):
    level, upper = row // 2, row % 2
    return level + upper * (2 * half - 1 - 2 * level)


def schedule(half, piece_time, link_delay, core_delay, backlog):
    free = {"ring0": 0.0, "ring1": 0.0, "side": 0.0, "core": 0.0}
    heap, order, serial, held = [], [], [0], ([], [])

    def post(now, link, key, size=1.0):
        span = size * (piece_time if link != "core" else piece_time / 8)
        begin = max(now, free[link])
        free[link] = begin + span
        delay = core_delay if link == "core" else link_delay
        serial[0] += 1
        heapq.heappush(heap, (begin + span + delay, serial[0], key))

    def ring(now, d, hop, chunk):
        post(now, "ring%d" % d, ("ring", d, hop, chunk), 0.5 if chunk > 4 else 1.0)
        order.append(("send", d, hop, chunk))

    def share(now, index):
        post(now, "core", ("core", index))
        post(now, "side", ("side", index))

    def release(now, limit):
        for d in (0, 1):
            while held[d] and free["ring%d" % d] - now < limit:
                ring(now, d, *held[d].pop(0))

    for d in (0, 1):
        ring(0.0, d, 1, 0)
    post(0.0, "core", ("pan", 0))
    for index in (1, 2):
        post(0.0, "side", ("pan", index))
    for d in (0, 1):
        ring(0.0, d, 1, 1)
    share(0.0, (0, 0))
    order.clear()
    while heap or held[0] or held[1]:
        if not heap:
            release(0.0, float("inf"))
        now, _, key = heapq.heappop(heap)
        order.append(key)
        if key[0] == "pan":
            for d in (0, 1):
                held[d].append((1, key[1] + 2))
        elif key[0] == "side":
            post(now, "core", ("pass", key[1]))
        elif key[0] == "ring":
            _, d, hop, chunk = key
            for onward in carried_on(half, FULL, SPLIT, d, hop, chunk):
                if onward == 0:
                    ring(now, d, hop + 1, 0)
                else:
                    held[d].append((hop + 1, onward))
            if chunk == 0:
                share(now, (d, hop))
        release(now, backlog)
    return order


def carried_on(half, full, split, d, hop, chunk):
    if hop + 1 < half:
        return (chunk,)
    if hop + 1 > half:
        return ()
    if chunk in split[d]:
        return (chunk,)
    return (5 + d,) if chunk == 3 else ()


FULL = (0, 1, 2, 3, 4)
SPLIT = ((0, 1, 5), (2, 4, 6))


def gather_kernel(
    ring, pattern_hbm, inverse, panel, diag, masked, coupled, held,
    pattern, g, m, pan, acc, tail,
    load_sem, ring_send, ring_recv, pan_send, pan_recv,
    core_send, core_recv, side_send, side_recv, pass_send, pass_recv,
):
    half = ring // 2
    row, col = lax.axis_index("prow"), lax.axis_index("pcol")
    place = position_of(row, half)
    rows, part = inverse.shape[1], inverse.shape[2]
    fine, width = panel.shape[1], masked.shape[2]
    order_rows = g.shape[1]
    core_mate = col + 1 - 2 * (col % 2)
    side_mate = lax.rem(col + 2, 4)
    far_mate = lax.rem(core_mate + 2, 4)
    forward = row_of(lax.rem(place + 1, ring), half)
    backward = row_of(lax.rem(place + ring - 1, ring), half)
    targets = ((forward, col), (backward, col))
    mates = (core_mate, side_mate, far_mate)
    sources = (col,) + mates

    def block_row(offset):
        return row_of(lax.rem(place + ring + offset, ring), half)

    def g_part(of_row, of_col):
        return g.at[
            :,
            pl.ds(pl.multiple_of(of_row * rows, rows), rows),
            pl.ds(pl.multiple_of(of_col * part, part), part),
        ]

    def m_part(of_row, of_col, first=0, count=2):
        start = pl.multiple_of(of_row * rows + of_col * fine, fine)
        return m.at[pl.ds(first, count), pl.ds(start, fine), :]

    def own_columns(of_col):
        return pan.at[:, :, pl.ds(pl.multiple_of(of_col * width, width), width)]

    load_panel = pltpu.make_async_copy(panel, pan, load_sem.at[0])
    load_g = pltpu.make_async_copy(inverse, g_part(row, col), load_sem.at[1])
    load_pattern = pltpu.make_async_copy(pattern_hbm, pattern, load_sem.at[2])
    load_g.start()
    load_panel.start()
    load_pattern.start()

    barrier = pltpu.get_barrier_semaphore()
    partners = targets + tuple((row, mate) for mate in mates)
    for partner in partners:
        pl.semaphore_signal(barrier, inc=1, device_id=partner, device_id_type=MESH)
    pl.semaphore_wait(barrier, len(partners))

    started = []

    def send(src, dst, send_sem, recv_sem, target):
        copy = pltpu.make_async_remote_copy(
            src_ref=src, dst_ref=dst, send_sem=send_sem, recv_sem=recv_sem,
            device_id=target, device_id_type=MESH,
        )
        copy.start()
        started.append(copy)

    def piece(offset, chunk):
        of_row = block_row(offset)
        if chunk == 0:
            return g_part(of_row, col)
        if chunk > 4:
            return m_part(of_row, side_mate, chunk - 5, 1)
        return m_part(of_row, sources[chunk - 1])

    def offset_of(key):
        return -key[1] if key[0] == 0 else key[1]

    def slot(key):
        return key[0] * half + key[1]

    def wait_recv(ref, sem):
        pltpu.make_async_copy(ref, ref, sem).wait()

    def ring_on(d, hop, chunk, src=None):
        ref = piece(offset_of((d, hop - 1)), chunk)
        send(
            ref if src is None else src, ref,
            ring_send.at[d, hop - 1, chunk], ring_recv.at[d, hop - 1, chunk], targets[d],
        )

    def share_g(key):
        ref, at = g_part(block_row(offset_of(key)), col), slot(key)
        send(ref, ref, core_send.at[at], core_recv.at[at], (row, core_mate))
        send(ref, ref, side_send.at[at], side_recv.at[at], (row, side_mate))

    def handle(key):
        if key[0] == "pan":
            wait_recv(m_part(row, mates[key[1]]), pan_recv.at[key[1]])
        elif key[0] == "send":
            ring_on(*key[1:])
        elif key[0] == "side":
            ref, at = g_part(block_row(offset_of(key[1])), side_mate), slot(key[1])
            wait_recv(ref, side_recv.at[at])
            send(ref, ref, pass_send.at[at], pass_recv.at[at], (row, core_mate))
        elif key[0] == "core":
            wait_recv(g_part(block_row(offset_of(key[1])), core_mate), core_recv.at[slot(key[1])])
        elif key[0] == "pass":
            wait_recv(g_part(block_row(offset_of(key[1])), far_mate), pass_recv.at[slot(key[1])])
        else:
            _, d, hop, chunk = key
            wait_recv(piece(offset_of((d, hop)), chunk), ring_recv.at[d, hop - 1, chunk])
            if chunk == 0:
                share_g((d, hop))

    load_g.wait()
    for d in (0, 1):
        ring_on(d, 1, 0)
    load_panel.wait()
    for index in (1, 2, 0):
        send(
            own_columns(mates[index]), m_part(row, col),
            pan_send.at[index], pan_recv.at[index], (row, mates[index]),
        )
    for d in (0, 1):
        ring_on(d, 1, 1, own_columns(col))
    share_g((0, 0))
    keep_own = pltpu.make_async_copy(own_columns(col), m_part(row, col), load_sem.at[3])
    keep_own.start()
    load_diag = pltpu.make_async_copy(diag, held, load_sem.at[4])
    load_diag.start()

    keys = schedule(half, 0.78, 1.65, 0.9, 1.0)
    last = [k for k in keys if k[0] == "ring" and k[2] == half and k[3] > 0]
    inert = [k for k in keys if k[0] in ("core", "pass")]
    for key in keys:
        if key not in last and key not in inert:
            handle(key)
    keep_own.wait()
    load_diag.wait()
    load_pattern.wait()

    super_index = col * width // WIDTH

    def rows_of(of_row):
        return pl.ds(pl.multiple_of(of_row * rows, rows), rows)

    def masked_rows(of_row):
        keep = pattern[of_row * rows // WIDTH, super_index] > 0
        values = m[:, rows_of(of_row), :]
        return jnp.where(keep, values, jnp.zeros_like(values))

    far_row = block_row(half)
    for offset in range(1 - half, half):
        of_row = block_row(offset)
        masked[:, rows_of(of_row), :] = masked_rows(of_row)
    masked[:, rows_of(far_row), :] = jnp.zeros((2, rows, width), masked.dtype)
    for key in inert:
        handle(key)

    step = min(256, width)
    for start in range(0, width, step):
        cols = slice(start, start + step)
        acc[0, :, cols] = dot(g[0], masked[0, :, cols], 1) - dot(g[1], masked[1, :, cols], 1)
        acc[1, :, cols] = dot(g[0], masked[1, :, cols], 1) + dot(g[1], masked[0, :, cols], 1)

    for key in last:
        handle(key)
    span = tail.shape[1]
    tail[...] = jnp.zeros_like(tail)
    far_values = masked_rows(far_row)
    masked[:, rows_of(far_row), :] = far_values
    tail[:, pl.ds(pl.multiple_of(lax.rem(far_row * rows, span), rows), rows), :] = far_values
    lanes = pl.ds(pl.multiple_of(far_row * rows // span * span, span), span)
    for start in range(0, width, step):
        cols = slice(start, start + step)
        real = acc[0, :, cols] + (
            dot(g[0, :, lanes], tail[0, :, cols], 1) - dot(g[1, :, lanes], tail[1, :, cols], 1)
        )
        imag = acc[1, :, cols] + (
            dot(g[0, :, lanes], tail[1, :, cols], 1) + dot(g[1, :, lanes], tail[0, :, cols], 1)
        )
        for block in range(order_rows // WIDTH):
            keep = (pattern[block, super_index] > 0).astype(jnp.float32)
            band = slice(block * WIDTH, (block + 1) * WIDTH)
            coupled[0, band, cols] = (real[band] * keep).astype(jnp.bfloat16)
            coupled[1, band, cols] = (imag[band] * keep).astype(jnp.bfloat16)
    for copy in started:
        copy.wait_send()


def dot(a, b, contract):
    return lax.dot_general(
        a, b, (((contract,), (0,)), ((), ())), preferred_element_type=jnp.float32
    )


def correct_kernel(masked, coupled, held, off_out, diag_out, off, total, save_sem):
    rows, height = off.shape[1], total.shape[1]
    row = lax.axis_index("prow")
    off[...] = -coupled[:, pl.ds(pl.multiple_of(row * rows, rows), rows), :]
    saves = [pltpu.make_async_copy(off, off_out, save_sem.at[0])]
    saves[0].start()
    step = min(128, height)
    for start in range(0, height, step):
        span = slice(start, start + step)
        for which in (0, 1):
            first = dot(masked[0, :, span], coupled[which], 0)
            second = dot(masked[1, :, span], coupled[1 - which], 0)
            total[which, span, :] = held[which, span, :] + (
                first - second if which == 0 else first + second
            )
            save = pltpu.make_async_copy(
                total.at[which, span, :], diag_out.at[which, span, :], save_sem.at[len(saves)]
            )
            save.start()
            saves.append(save)
    for save in saves:
        save.wait()


def in_hbm(array):
    return pltpu.with_memory_space_constraint(array, pltpu.HBM)


def gathered(inverse_block, panel, pattern, diag_inverse):
    ring = lax.axis_size("prow")
    half = ring // 2
    rows = inverse_block.shape[1]
    order, width, height = rows * ring, diag_inverse.shape[2], diag_inverse.shape[1]
    dma = pltpu.SemaphoreType.DMA
    anywhere = pl.BlockSpec(memory_space=pl.ANY)
    whole = pl.BlockSpec(memory_space=pltpu.VMEM)
    tall = jax.ShapeDtypeStruct((2, order, width), jnp.bfloat16)
    masked, coupled, held = pl.pallas_call(
        functools.partial(gather_kernel, ring),
        out_shape=(tall, tall, jax.ShapeDtypeStruct(diag_inverse.shape, jnp.float32)),
        in_specs=[anywhere] * 4,
        out_specs=(whole,) * 3,
        scratch_shapes=[
            pltpu.SMEM(pattern.shape, jnp.int32),
            pltpu.VMEM((2, order, order), jnp.bfloat16),
            pltpu.VMEM((2, order, width), jnp.bfloat16),
            pltpu.VMEM(panel.shape, jnp.bfloat16),
            pltpu.VMEM((2, order, width), jnp.float32),
            pltpu.VMEM((2, max(rows, 128), width), jnp.bfloat16),
            dma((5,)),
            dma((2, half, 7)), dma((2, half, 7)),
            dma((3,)), dma((3,)),
            dma((ring + 1,)), dma((ring + 1,)),
            dma((ring + 1,)), dma((ring + 1,)),
            dma((ring + 1,)), dma((ring + 1,)),
        ],
        compiler_params=pltpu.CompilerParams(
            collective_id=0, has_side_effects=True, vmem_limit_bytes=VMEM_BUDGET
        ),
    )(in_hbm(pattern), in_hbm(inverse_block), in_hbm(panel), in_hbm(diag_inverse))
    return pl.pallas_call(
        correct_kernel,
        out_shape=(
            jax.ShapeDtypeStruct((2, rows, width), jnp.bfloat16),
            jax.ShapeDtypeStruct(diag_inverse.shape, jnp.float32),
        ),
        in_specs=[whole] * 3,
        out_specs=(anywhere, anywhere),
        scratch_shapes=[
            pltpu.VMEM((2, rows, width), jnp.bfloat16),
            pltpu.VMEM(diag_inverse.shape, jnp.float32),
            dma((2 * pl.cdiv(height, 128) + 1,)),
        ],
        compiler_params=pltpu.CompilerParams(vmem_limit_bytes=VMEM_BUDGET),
    )(masked, coupled, held)


def fits(ring, col_count, inverse_block, panel, diag_inverse):
    rows, width = inverse_block.shape[1], diag_inverse.shape[2]
    order = rows * ring
    held = 4 * order * order + 8 * order * width + 16 * diag_inverse.shape[1] * width
    return (
        ring % 2 == 0 and ring >= 4 and col_count == 4 and width == WIDTH
        and panel.shape[1] % 16 == 0 and inverse_block.shape[2] % 128 == 0
        and order % WIDTH == 0 and max(rows, 128) % rows == 0 and rows % 16 == 0
        and WIDTH % rows == 0 and held <= VMEM_BUDGET * 2 // 3
    )


def complex_product(left_real, left_imag, right_real, right_imag, contract):
    dims = (((contract,), (0,)), ((), ()))
    real_part = lax.dot_general(
        left_real, right_real, dims, preferred_element_type=jnp.float32
    ) - lax.dot_general(left_imag, right_imag, dims, preferred_element_type=jnp.float32)
    imag_part = lax.dot_general(
        left_real, right_imag, dims, preferred_element_type=jnp.float32
    ) + lax.dot_general(left_imag, right_real, dims, preferred_element_type=jnp.float32)
    return (real_part, imag_part)


def keep_table(pattern, row_start, row_count, col_start, col_count, block_width):
    row_ids = (row_start + jnp.arange(row_count, dtype=jnp.int32)) // block_width
    col_ids = (col_start + jnp.arange(col_count, dtype=jnp.int32)) // block_width
    row_select = (
        row_ids[:, None] == jnp.arange(pattern.shape[0], dtype=jnp.int32)[None, :]
    ).astype(jnp.float32)
    col_select = (
        col_ids[:, None] == jnp.arange(pattern.shape[1], dtype=jnp.int32)[None, :]
    ).astype(jnp.float32)
    pattern_value = pattern.astype(jnp.float32)
    row_pattern = jnp.dot(row_select, pattern_value, precision=lax.Precision.HIGHEST)
    return jnp.dot(row_pattern, col_select.T, precision=lax.Precision.HIGHEST)


def local(inverse_block, panel, pattern, diag_inverse):
    rows_dev = inverse_block.shape[1]
    block_span = inverse_block.shape[2]
    fine_rows = panel.shape[1]
    columns = panel.shape[2]
    if fits(lax.axis_size("prow"), lax.axis_size("pcol"), inverse_block, panel, diag_inverse):
        return gathered(inverse_block, panel, pattern, diag_inverse)
    row_index = lax.axis_index("prow")
    col_index = lax.axis_index("pcol")
    col_count = lax.axis_size("pcol")
    root_count = lax.axis_size("prow") // col_count
    fine_start = (row_index * col_count + col_index) * fine_rows
    keep_mask = keep_table(pattern, fine_start, fine_rows, 0, columns, WIDTH)
    masked = jnp.where(keep_mask[None] > 0.5, panel, jnp.zeros_like(panel))
    row_panel = lax.all_gather(masked, "pcol", axis=1, tiled=True)
    flipped = jnp.swapaxes(inverse_block, 1, 2)
    split_cols = flipped.reshape(2, root_count, col_count, fine_rows, rows_dev)
    received = lax.all_to_all(split_cols, "pcol", split_axis=2, concat_axis=1, tiled=True)
    regrouped = received.reshape(2, block_span, rows_dev)
    panel_piece = lax.all_gather(masked, "prow", axis=1, tiled=True)
    part_real, part_imag = complex_product(
        regrouped[0], regrouped[1], panel_piece[0], panel_piece[1], 0
    )
    stacked = jnp.stack([part_real, part_imag])
    summed = lax.psum_scatter(stacked, "pcol", scatter_dimension=2, tiled=True)
    local_cols = summed.shape[2]
    keep_local = keep_table(
        pattern, row_index * rows_dev, rows_dev, col_index * local_cols, local_cols, WIDTH
    )
    coupled = (summed * keep_local[None]).astype(jnp.bfloat16)
    offdiag = -coupled
    block_start = col_index * local_cols // WIDTH * WIDTH
    lower_panel = lax.dynamic_slice_in_dim(row_panel, block_start, WIDTH, 2)
    diag_real, diag_imag = complex_product(
        lower_panel[0], lower_panel[1], coupled[0], coupled[1], 0
    )
    shares = lax.psum_scatter(
        jnp.stack([diag_real, diag_imag]), "prow", scatter_dimension=1, tiled=True
    )
    correction = lax.all_gather(shares, "prow", axis=1, tiled=True)
    return (offdiag, diag_inverse + correction)


def solution(mesh):
    in_specs = (
        P(None, "prow", "pcol"),
        P(None, ("prow", "pcol"), None),
        P(),
        P(None, None, "pcol"),
    )
    out_specs = (P(None, "prow", "pcol"), P(None, None, "pcol"))
    return jax.shard_map(local, mesh=mesh, in_specs=in_specs, out_specs=out_specs, check_vma=False)
```
